32 devices in a mesh: dp: 1 (over z), sp: 32 (over y, x, core).
Axes of the slice: x: 4, y: 4, z: 1, core: 2. Of those that a mesh axis runs over, the one named last changes fastest.
The devices are a block of a 4x4x8 slice.
Arguments:
- latent: bfloat16 [16, 128, 128, 4], P('dp', 'sp')
- time_emb: bfloat16 [16, 1280], P('dp')
- w_in: bfloat16 [3, 3, 4, 320], replicated
- b_in: bfloat16 [320], replicated
- gn1_scale: bfloat16 [2, 320], replicated
- gn1_shift: bfloat16 [2, 320], replicated
- conv1_w: bfloat16 [2, 3, 3, 320, 320], replicated
- conv1_b: bfloat16 [2, 320], replicated
- temb_w: bfloat16 [2, 1280, 320], replicated
- temb_b: bfloat16 [2, 320], replicated
- gn2_scale: bfloat16 [2, 320], replicated
- gn2_shift: bfloat16 [2, 320], replicated
- conv2_w: bfloat16 [2, 3, 3, 320, 320], replicated
- conv2_b: bfloat16 [2, 320], replicated
- down_w: bfloat16 [3, 3, 320, 320], replicated
- down_b: bfloat16 [320], replicated
Outputs:
- output 1: bfloat16 [16, 128, 128, 320], P('dp', 'sp')
- output 2: bfloat16 [16, 128, 128, 320], P('dp', 'sp')
- output 3: bfloat16 [16, 128, 128, 320], P('dp', 'sp')
- output 4: bfloat16 [16, 64, 64, 320], P('dp', 'sp')
All inputs are finite; a program needn't handle non-finite values.
Results may differ from the reference program's by a relative error of at most 0.0134259.
Values are sent between devices in bfloat16 or wider.
A program may use at most 768 MiB of HBM per device.

```python
import jax
import jax.numpy as jnp
from jax import lax

BATCH = 16
HEIGHT = 128
WIDTH = 128
CHANNELS = 320
TEMB_DIM = 1280
LATENT_CH = 4
GROUPS = 32
LAYERS = 2
GN_EPS = 1e-5


def setup_inputs(seed: int = 0, part: int = 0) -> dict:
    part_keys = jax.random.split(jax.random.fold_in(jax.random.key(seed), part), 4)
    shared_keys = jax.random.split(jax.random.key(seed + 1), 14)
    row_pos = jnp.linspace(-1.0, 1.0, HEIGHT)[None, :, None, None]
    noise_part = jax.random.normal(part_keys[0], (BATCH, HEIGHT, WIDTH, LATENT_CH), jnp.float32)
    row_slope = 1.5 * jax.random.normal(part_keys[1], (BATCH, 1, 1, LATENT_CH), jnp.float32)
    row_curve = jax.random.normal(part_keys[2], (BATCH, 1, 1, LATENT_CH), jnp.float32)
    latent = noise_part + row_slope * row_pos + row_curve * (1.5 * row_pos * row_pos - 0.5)
    time_emb = jax.random.normal(part_keys[3], (BATCH, TEMB_DIM), jnp.float32)
    conv_std = 1.2 * (9 * CHANNELS) ** -0.5

    def draw_w(key_slot, arr_shape, spread, center):
        return (center + spread * jax.random.normal(shared_keys[key_slot], arr_shape, jnp.float32)).astype(jnp.bfloat16)

    return {
        "latent": latent.astype(jnp.bfloat16),
        "time_emb": time_emb.astype(jnp.bfloat16),
        "w_in": draw_w(0, (3, 3, LATENT_CH, CHANNELS), (9 * LATENT_CH) ** -0.5, 0.0),
        "b_in": draw_w(1, (CHANNELS,), 0.5, 0.0),
        "gn1_scale": draw_w(2, (LAYERS, CHANNELS), 0.3, 1.0),
        "gn1_shift": draw_w(3, (LAYERS, CHANNELS), 0.3, 0.0),
        "conv1_w": draw_w(4, (LAYERS, 3, 3, CHANNELS, CHANNELS), conv_std, 0.0),
        "conv1_b": draw_w(5, (LAYERS, CHANNELS), 0.3, 0.0),
        "temb_w": draw_w(6, (LAYERS, TEMB_DIM, CHANNELS), TEMB_DIM ** -0.5, 0.0),
        "temb_b": draw_w(7, (LAYERS, CHANNELS), 0.3, 0.0),
        "gn2_scale": draw_w(8, (LAYERS, CHANNELS), 0.3, 1.0),
        "gn2_shift": draw_w(9, (LAYERS, CHANNELS), 0.3, 0.0),
        "conv2_w": draw_w(10, (LAYERS, 3, 3, CHANNELS, CHANNELS), conv_std, 0.0),
        "conv2_b": draw_w(11, (LAYERS, CHANNELS), 0.3, 0.0),
        "down_w": draw_w(12, (3, 3, CHANNELS, CHANNELS), (9 * CHANNELS) ** -0.5, 0.0),
        "down_b": draw_w(13, (CHANNELS,), 0.3, 0.0),
    }


def conv_same(inputs, kernel, bias_c, stride):
    out_f32 = lax.conv_general_dilated(inputs[None].astype(jnp.float32), kernel.astype(jnp.float32), (stride, stride), ((1, 1), (1, 1)), dimension_numbers=("NHWC", "HWIO", "NHWC"))
    return (out_f32[0] + bias_c.astype(jnp.float32)).astype(jnp.bfloat16)


def norm_silu(values, gain_c, shift_c):
    grouped = values.reshape(values.shape[0] * values.shape[1], GROUPS, CHANNELS // GROUPS)
    grp_mean = jnp.mean(grouped, axis=(0, 2), keepdims=True)
    grp_var = jnp.mean(jnp.square(grouped - grp_mean), axis=(0, 2), keepdims=True)
    normed = ((grouped - grp_mean) * lax.rsqrt(grp_var + GN_EPS)).reshape(values.shape)
    normed = normed * gain_c.astype(jnp.float32) + shift_c.astype(jnp.float32)
    return jax.nn.silu(normed).astype(jnp.bfloat16)


def reference(latent, time_emb, w_in, b_in, gn1_scale, gn1_shift, conv1_w, conv1_b, temb_w, temb_b, gn2_scale, gn2_shift, conv2_w, conv2_b, down_w, down_b):
    layer_params = (gn1_scale, gn1_shift, conv1_w, conv1_b, temb_w, temb_b, gn2_scale, gn2_shift, conv2_w, conv2_b)

    def one_sample(sample):
        latent_s, temb_s = sample
        first_out = conv_same(latent_s, w_in, b_in, 1)
        emb_act = jax.nn.silu(temb_s.astype(jnp.float32)).astype(jnp.bfloat16)

        def layer_step(hidden, params):
            norm_g1, norm_b1, conv_w1, conv_b1, proj_w, proj_b, norm_g2, norm_b2, conv_w2, conv_b2 = params
            branch = conv_same(norm_silu(hidden.astype(jnp.float32), norm_g1, norm_b1), conv_w1, conv_b1, 1)
            emb_proj = jnp.dot(emb_act.astype(jnp.float32), proj_w.astype(jnp.float32)) + proj_b.astype(jnp.float32)
            mixed_in = branch.astype(jnp.float32) + emb_proj
            branch = conv_same(norm_silu(mixed_in, norm_g2, norm_b2), conv_w2, conv_b2, 1)
            hidden = (hidden.astype(jnp.float32) + branch.astype(jnp.float32)).astype(jnp.bfloat16)
            return hidden, hidden

        last_out, per_layer = lax.scan(layer_step, first_out, layer_params)
        return first_out, per_layer, conv_same(last_out, down_w, down_b, 2)

    firsts, layers_out, down_outs = lax.map(one_sample, (latent, time_emb))
    return firsts, layers_out[:, 0], layers_out[:, 1], down_outs
```

```python
import functools

import jax
import jax.numpy as jnp
from jax import lax
from jax.experimental import pallas as pl
from jax.experimental.pallas import tpu as pltpu
from jax.sharding import PartitionSpec as P

GN_GROUPS = 32
GN_EPS = 1e-5
QUAD = 4
LATENT_PAD = 16
MESH_ID = pl.DeviceIdType.MESH
F32 = jnp.float32
BF16 = jnp.bfloat16

COL_BIN, COL_BDOWN = 0, 1
COL_G1, COL_S1, COL_B1, COL_G2, COL_S2, COL_B2 = 2, 4, 6, 8, 10, 12
N_COLS = 14


def band_kernel(
    n_sp, axis,
    lat_hbm, win_ref, w1_hbm, w2_hbm, wd_hbm, par_ref, emb_ref, sel_ref,
    h0_hbm, h1_hbm, h2_hbm, d_hbm,
    lat, xl, hb, ub, xb, w1, w2, wd, bc, stat, scl, ofs, inv_b, mean_b, sbuf, rbuf, dbuf,
    lat_sem, w_sem, out_sem, d_sem, latx_send, latx_recv, st_send, st_recv, u_send, u_recv, h_send, h_recv,
):
    n_quad, _, chan, lanes = hb.shape
    cols = lanes // QUAD
    group_ch = chan // GN_GROUPS
    kk = 3 * chan
    rows = h0_hbm.shape[1]
    chunk = 80
    me = lax.axis_index(axis)
    above = lax.rem(me + n_sp - 1, n_sp)
    below = lax.rem(me + 1, n_sp)
    has_above = me > 0
    has_below = me < n_sp - 1
    count = float(rows * n_sp * cols * group_ch)

    def peer(dist):
        return lax.rem(me + dist, n_sp)

    lat_load = pltpu.make_async_copy(lat_hbm, lat.at[:, 2 : 2 + rows], lat_sem)
    lat_load.start()
    w_loads = [
        pltpu.make_async_copy(w1_hbm.at[0], w1.at[0], w_sem.at[0]),
        pltpu.make_async_copy(w2_hbm.at[0], w2.at[0], w_sem.at[1]),
        pltpu.make_async_copy(w1_hbm.at[1], w1.at[1], w_sem.at[2]),
        pltpu.make_async_copy(w2_hbm.at[1], w2.at[1], w_sem.at[3]),
        pltpu.make_async_copy(wd_hbm, wd, w_sem.at[4]),
    ]
    for load in w_loads:
        load.start()

    barrier = pltpu.get_barrier_semaphore()

    @pl.loop(1, n_sp)
    def _(dist):
        pl.semaphore_signal(barrier, inc=1, device_id={axis: peer(dist)}, device_id_type=MESH_ID)

    pl.semaphore_wait(barrier, n_sp - 1)

    lat_down = pltpu.make_async_remote_copy(
        lat_hbm.at[:, rows - 2 : rows], lat.at[:, 0:2], latx_send.at[0], latx_recv.at[0], device_id={axis: below}, device_id_type=MESH_ID)
    lat_up = pltpu.make_async_remote_copy(
        lat_hbm.at[:, 0:2], lat.at[:, 2 + rows : 4 + rows], latx_send.at[1], latx_recv.at[1], device_id={axis: above}, device_id_type=MESH_ID)
    lat_down.start()
    lat_up.start()

    for col in range(N_COLS):
        bc[col] = jnp.broadcast_to(par_ref[:, col : col + 1], (chan, cols))

    lane_id = lax.broadcasted_iota(jnp.int32, (chunk, cols), 1)
    lane_id_small = lax.broadcasted_iota(jnp.int32, (LATENT_PAD, cols), 1)

    def store_taps(dst, base, stride, c0, size, k, val, ids):
        left = jnp.where(ids == 0, 0.0, pltpu.roll(val, 1, 1))
        right = jnp.where(ids == cols - 1, 0.0, pltpu.roll(val, cols - 1, 1))
        for tap, piece in enumerate((left, val, right)):
            dst[pl.ds(base + tap * stride + c0, size), k * cols : (k + 1) * cols] = piece.astype(BF16)

    def zero_stats():
        stat[...] = jnp.zeros_like(stat)

    def add_stats(k, c0, val):
        stat[k, pl.ds(c0, chunk), :] += val
        stat[QUAD + k, pl.ds(c0, chunk), :] += val * val

    def stats_copy(par, q, dist):
        return pltpu.make_async_remote_copy(
            sbuf.at[par, q], rbuf.at[par, q, dist - 1], st_send.at[par, q], st_recv.at[par, q],
            device_id={axis: peer(dist)}, device_id_type=MESH_ID)

    def send_stats(par, q):
        lane32 = lax.broadcasted_iota(jnp.int32, (GN_GROUPS, cols), 1)
        packed = jnp.zeros((GN_GROUPS, cols), F32)
        for idx in range(2 * QUAD):
            ref = stat.at[idx]
            group = ref[pl.ds(0, GN_GROUPS, stride=group_ch), :]
            for j in range(1, group_ch):
                group = group + ref[pl.ds(j, GN_GROUPS, stride=group_ch), :]
            packed = jnp.where(lane32 == idx, jnp.sum(group, axis=1, keepdims=True), packed)
        square = jnp.concatenate([packed, jnp.zeros((cols - GN_GROUPS, cols), F32)], axis=0)
        sbuf[par, q] = jnp.transpose(square)[: 2 * QUAD, :]

        @pl.loop(1, n_sp)
        def _(dist):
            stats_copy(par, q, dist).start()

    def wait_stats(par, q):
        whole = pltpu.make_async_remote_copy(
            rbuf.at[par, q], rbuf.at[par, q], st_send.at[par, q], st_recv.at[par, q],
            device_id={axis: below}, device_id_type=MESH_ID)
        whole.wait_send()
        whole.wait_recv()

    def make_scale(par, q, col_g, col_s, emb_idx):
        total = sbuf[par, q]
        for d in range(n_sp - 1):
            total = total + rbuf[par, q, d]
        mean = total[:QUAD] / count
        var = total[QUAD:] / count - mean * mean
        inv = lax.rsqrt(var + GN_EPS)
        square = jnp.concatenate([mean, inv, jnp.zeros((cols - 2 * QUAD, cols), F32)], axis=0)
        flipped = jnp.transpose(square)[:GN_GROUPS, :]
        for k in range(QUAD):
            mean_k = jnp.broadcast_to(flipped[:, k : k + 1], (GN_GROUPS, cols))
            inv_k = jnp.broadcast_to(flipped[:, QUAD + k : QUAD + k + 1], (GN_GROUPS, cols))
            for j in range(group_ch):
                mean_b.at[k][pl.ds(j, GN_GROUPS, stride=group_ch), :] = mean_k
                inv_b.at[k][pl.ds(j, GN_GROUPS, stride=group_ch), :] = inv_k
        for k in range(QUAD):
            for c0 in range(0, chan, chunk):
                cs = pl.ds(c0, chunk)
                half_scale = inv_b[k, cs, :] * (0.5 * bc[col_g, cs, :])
                center = mean_b[k, cs, :]
                if emb_idx is not None:
                    center = center - emb_ref[emb_idx, cs, k : k + 1]
                scl[k, cs, :] = half_scale
                ofs[k, cs, :] = 0.5 * bc[col_s, cs, :] - center * half_scale

    def norm_rows(src, q):
        @pl.loop(0, rows + 2)
        def _(row):
            keep = jnp.logical_and(jnp.logical_or(row > 0, has_above), jnp.logical_or(row < rows + 1, has_below))
            flag = keep.astype(jnp.int32)
            for k in range(QUAD):
                for c0 in range(0, chan, chunk):
                    val = src[q, row, pl.ds(c0, chunk), k * cols : (k + 1) * cols].astype(F32)
                    half = val * scl[k, pl.ds(c0, chunk), :] + ofs[k, pl.ds(c0, chunk), :]
                    half = jnp.where(flag > 0, half, 0.0)
                    act = half + half * jnp.tanh(half)
                    store_taps(xb, row * kk, chan, c0, chunk, k, act, lane_id)

    def halo_copies(buf, send, recv, q):
        down = pltpu.make_async_remote_copy(
            buf.at[q, rows], buf.at[q, 0], send.at[q, 0], recv.at[q, 0], device_id={axis: below}, device_id_type=MESH_ID)
        up = pltpu.make_async_remote_copy(
            buf.at[q, 1], buf.at[q, rows + 1], send.at[q, 1], recv.at[q, 1], device_id={axis: above}, device_id_type=MESH_ID)
        return down, up

    def send_halo(buf, send, recv, q):
        for copy in halo_copies(buf, send, recv, q):
            copy.start()

    def wait_halo(buf, send, recv, q):
        for copy in halo_copies(buf, send, recv, q):
            copy.wait()

    def out_copies(dst, q):
        return [
            pltpu.make_async_copy(hb.at[q, 1 : 1 + rows, :, k * cols : (k + 1) * cols], dst.at[q * QUAD + k], out_sem.at[q, k])
            for k in range(QUAD)
        ]

    lat_load.wait()
    lat_down.wait()
    lat_up.wait()

    @pl.loop(0, n_quad)
    def _(q):
        for row in range(rows + 4):
            for k in range(QUAD):
                val = lat[q, row, :, k * cols : (k + 1) * cols].astype(F32)
                if row < 2:
                    val = jnp.where(has_above, val, 0.0)
                if row >= rows + 2:
                    val = jnp.where(has_below, val, 0.0)
                store_taps(xl, row * 3 * LATENT_PAD, LATENT_PAD, 0, LATENT_PAD, k, val, lane_id_small)
        zero_stats()
        for row in range(rows + 2):
            acc = jnp.dot(win_ref[...], xl[row * 3 * LATENT_PAD : (row + 3) * 3 * LATENT_PAD, :], preferred_element_type=F32)
            for k in range(QUAD):
                for c0 in range(0, chan, chunk):
                    val = (acc[c0 : c0 + chunk, k * cols : (k + 1) * cols] + bc[COL_BIN, c0 : c0 + chunk, :]).astype(BF16)
                    hb[q, row, c0 : c0 + chunk, k * cols : (k + 1) * cols] = val
                    if 1 <= row <= rows:
                        add_stats(k, c0, val.astype(F32))
        send_stats(0, q)
        for copy in out_copies(h0_hbm, q):
            copy.start()

    @pl.loop(0, w1.shape[0])
    def _(layer):
        for idx in range(w1.shape[0]):
            @pl.when(layer == idx)
            def _():
                w_loads[2 * idx].wait()

        @pl.loop(0, n_quad)
        def _(q):
            wait_stats(0, q)

            @pl.when(layer > 0)
            def _():
                wait_halo(hb, h_send, h_recv, q)

            make_scale(0, q, COL_G1 + layer, COL_S1 + layer, None)
            norm_rows(hb, q)
            zero_stats()

            @pl.loop(0, rows)
            def _(row):
                acc = jnp.dot(w1[layer], xb[pl.ds(row * kk, 3 * kk), :], preferred_element_type=F32)
                for k in range(QUAD):
                    for c0 in range(0, chan, chunk):
                        cs = pl.ds(c0, chunk)
                        val = (acc[c0 : c0 + chunk, k * cols : (k + 1) * cols] + bc[COL_B1 + layer, cs, :]).astype(BF16)
                        ub[q, row + 1, cs, k * cols : (k + 1) * cols] = val
                        add_stats(k, c0, val.astype(F32) + emb_ref[layer * n_quad + q, cs, k : k + 1])

            send_halo(ub, u_send, u_recv, q)
            send_stats(1, q)

        for idx in range(w1.shape[0]):
            @pl.when(layer == idx)
            def _():
                w_loads[2 * idx + 1].wait()

        @pl.loop(0, n_quad)
        def _(q):
            wait_stats(1, q)
            wait_halo(ub, u_send, u_recv, q)
            make_scale(1, q, COL_G2 + layer, COL_S2 + layer, layer * n_quad + q)
            norm_rows(ub, q)
            zero_stats()
            for copy in out_copies(h0_hbm, q):
                copy.wait()

            @pl.loop(0, rows)
            def _(row):
                acc = jnp.dot(w2[layer], xb[pl.ds(row * kk, 3 * kk), :], preferred_element_type=F32)
                for k in range(QUAD):
                    for c0 in range(0, chan, chunk):
                        cs = pl.ds(c0, chunk)
                        branch = (acc[c0 : c0 + chunk, k * cols : (k + 1) * cols] + bc[COL_B2 + layer, cs, :]).astype(BF16).astype(F32)
                        val = (hb[q, row + 1, cs, k * cols : (k + 1) * cols].astype(F32) + branch).astype(BF16)
                        hb[q, row + 1, cs, k * cols : (k + 1) * cols] = val
                        add_stats(k, c0, val.astype(F32))

            send_halo(hb, h_send, h_recv, q)

            @pl.when(layer == 0)
            def _():
                send_stats(0, q)
                for copy in out_copies(h1_hbm, q):
                    copy.start()

            @pl.when(layer > 0)
            def _():
                for copy in out_copies(h2_hbm, q):
                    copy.start()

    w_loads[4].wait()

    def d_copies(q):
        return [pltpu.make_async_copy(dbuf.at[q, k], d_hbm.at[q * QUAD + k], d_sem.at[q, k]) for k in range(QUAD)]

    @pl.loop(0, n_quad)
    def _(q):
        wait_halo(hb, h_send, h_recv, q)

        @pl.loop(0, rows + 1)
        def _(row):
            keep = jnp.logical_or(row > 0, has_above)
            flag = keep.astype(jnp.int32)
            for k in range(QUAD):
                for c0 in range(0, chan, chunk):
                    val = hb[q, row, pl.ds(c0, chunk), k * cols : (k + 1) * cols].astype(F32)
                    val = jnp.where(flag > 0, val, 0.0)
                    store_taps(xb, row * kk, chan, c0, chunk, k, val, lane_id)

        @pl.loop(0, rows // 2)
        def _(row):
            acc = jnp.dot(wd[...], xb[pl.ds(2 * row * kk, 3 * kk), :], preferred_element_type=F32)
            for k in range(QUAD):
                full = (acc[:, k * cols : (k + 1) * cols] + bc[COL_BDOWN]).astype(BF16)
                picked = lax.dot_general(sel_ref[...], full, (((1,), (1,)), ((), ())), preferred_element_type=F32)
                dbuf[q, k, row] = picked.astype(BF16)

        for copy in d_copies(q):
            copy.start()

    @pl.loop(0, n_quad)
    def _(q):
        for copy in out_copies(h2_hbm, q):
            copy.wait()
        for copy in d_copies(q):
            copy.wait()


def solution(mesh):
    n_sp = mesh.shape["sp"]

    def band_program(latent, time_emb, w_in, b_in, gn1_scale, gn1_shift, conv1_w, conv1_b, temb_w, temb_b, gn2_scale, gn2_shift, conv2_w, conv2_b, down_w, down_b):
        batch, rows, cols, lat_ch = latent.shape
        chan = w_in.shape[-1]
        layers = conv1_w.shape[0]
        n_quad = batch // QUAD
        lanes = QUAD * cols
        kk = 3 * chan

        lat = latent.reshape(n_quad, QUAD, rows, cols, lat_ch).transpose(0, 2, 4, 1, 3).reshape(n_quad, rows, lat_ch, lanes)
        lat = jnp.pad(lat, ((0, 0), (0, 0), (0, LATENT_PAD - lat_ch), (0, 0)))
        win = jnp.pad(w_in, ((0, 0), (0, 0), (0, LATENT_PAD - lat_ch), (0, 0))).reshape(9 * LATENT_PAD, chan).T
        w1 = conv1_w.reshape(layers, 9 * chan, chan).transpose(0, 2, 1)
        w2 = conv2_w.reshape(layers, 9 * chan, chan).transpose(0, 2, 1)
        wd = down_w.reshape(9 * chan, chan).T
        par = jnp.concatenate([b_in[None], down_b[None], gn1_scale, gn1_shift, conv1_b, gn2_scale, gn2_shift, conv2_b], axis=0).astype(F32).T
        emb_act = jax.nn.silu(time_emb.astype(F32)).astype(BF16)
        emb = jnp.einsum("bt,ltc->lbc", emb_act, temb_w, preferred_element_type=F32) + temb_b.astype(F32)[:, None, :]
        emb = emb.reshape(layers * n_quad, QUAD, chan).transpose(0, 2, 1)
        sel = (lax.broadcasted_iota(jnp.int32, (cols // 2, cols), 1) == 2 * lax.broadcasted_iota(jnp.int32, (cols // 2, cols), 0)).astype(BF16)

        band = jax.ShapeDtypeStruct((batch, rows, chan, cols), BF16)
        hbm = pl.BlockSpec(memory_space=pl.ANY)
        vmem = pl.BlockSpec(memory_space=pltpu.VMEM)
        dma = pltpu.SemaphoreType.DMA
        h0, h1, h2, d = pl.pallas_call(
            functools.partial(band_kernel, n_sp, "sp"),
            out_shape=(band, band, band, jax.ShapeDtypeStruct((batch, rows // 2, cols // 2, chan), BF16)),
            in_specs=[hbm, vmem, hbm, hbm, hbm, vmem, vmem, vmem],
            out_specs=(hbm,) * 4,
            scratch_shapes=[
                pltpu.VMEM((n_quad, rows + 4, LATENT_PAD, lanes), BF16),
                pltpu.VMEM(((rows + 4) * 3 * LATENT_PAD, lanes), BF16),
                pltpu.VMEM((n_quad, rows + 2, chan, lanes), BF16),
                pltpu.VMEM((n_quad, rows + 2, chan, lanes), BF16),
                pltpu.VMEM(((rows + 2) * kk, lanes), BF16),
                pltpu.VMEM((layers, chan, 9 * chan), BF16),
                pltpu.VMEM((layers, chan, 9 * chan), BF16),
                pltpu.VMEM((chan, 9 * chan), BF16),
                pltpu.VMEM((N_COLS, chan, cols), F32),
                pltpu.VMEM((2 * QUAD, chan, cols), F32),
                pltpu.VMEM((QUAD, chan, cols), F32),
                pltpu.VMEM((QUAD, chan, cols), F32),
                pltpu.VMEM((QUAD, chan, cols), F32),
                pltpu.VMEM((QUAD, chan, cols), F32),
                pltpu.VMEM((2, n_quad, 2 * QUAD, cols), F32),
                pltpu.VMEM((2, n_quad, n_sp - 1, 2 * QUAD, cols), F32),
                pltpu.VMEM((n_quad, QUAD, rows // 2, cols // 2, chan), BF16),
                dma, dma((5,)), dma((n_quad, QUAD)), dma((n_quad, QUAD)),
                dma((2,)), dma((2,)), dma((2, n_quad)), dma((2, n_quad)),
                dma((n_quad, 2)), dma((n_quad, 2)), dma((n_quad, 2)), dma((n_quad, 2)),
            ],
            compiler_params=pltpu.CompilerParams(collective_id=0, has_side_effects=True, vmem_limit_bytes=60 * 1024 * 1024),
            name="band",
        )(lat, win, w1, w2, wd, par, emb, sel)
        return tuple(h.transpose(0, 1, 3, 2) for h in (h0, h1, h2)) + (d,)

    band_spec = P("dp", "sp", None, None)
    return jax.shard_map(band_program, mesh=mesh, in_specs=(band_spec, P("dp", None)) + (P(),) * 14, out_specs=(band_spec,) * 4, check_vma=False)
```

```python
import functools

import jax
import jax.numpy as jnp
from jax import lax
from jax.experimental import pallas as pl
from jax.experimental.pallas import tpu as pltpu
from jax.sharding import PartitionSpec as P

GN_GROUPS = 32
GN_EPS = 1e-5
QUAD = 4
LATENT_PAD = 16
CORES = 2
MESH_ID = pl.DeviceIdType.MESH
F32 = jnp.float32
BF16 = jnp.bfloat16

COL_BIN = 0
COL_G1, COL_S1, COL_B1, COL_G2, COL_S2, COL_B2 = 1, 3, 5, 7, 9, 11
COL_BDOWN = 13
N_COLS = 13


def store_shifts(dst, base, stride, k, val):
    size, cols = val.shape
    lane = lax.broadcasted_iota(jnp.int32, val.shape, 1)
    zero = jnp.zeros_like(val)
    left = jnp.where(lane == 0, zero, pltpu.roll(val, 1, 1))
    right = jnp.where(lane == cols - 1, zero, pltpu.roll(val, cols - 1, 1))
    for tap, piece in enumerate((left, val, right)):
        dst[base + tap * stride : base + tap * stride + size, k * cols : (k + 1) * cols] = piece


def transpose_weight(raw, out):
    for start in range(0, out.shape[1], 128):
        out[:, start : start + 128] = jnp.transpose(raw[start : start + 128, :])


def band_kernel(
    n_sp, axis,
    lat_hbm, win_ref, w1_hbm, w2_hbm, wd_hbm, par_ref, emb_ref,
    h0_hbm, h1_hbm, h2_hbm, halo_hbm, wt_hbm,
    lat, xl, act, xb0, xb1, raw, wt, acc_a, acc_b, bc, stat_a, stat_b, scl, ofs, inv_b, mean_b, sbuf_a, rbuf_a, sbuf, rbuf,
    lat_sem, w_sem, wt_sem, out_sem, d_sem, latx_send, latx_recv, sa_send, sa_recv, st_send, st_recv, x_send, x_recv,
):
    _, n_quad, _, chan, lanes = act.shape
    cols = lanes // QUAD
    group_ch = chan // GN_GROUPS
    kk = 3 * chan
    rows = h0_hbm.shape[1]
    chunk = 80
    me = lax.axis_index(axis)
    above = lax.rem(me + n_sp - 1, n_sp)
    below = lax.rem(me + 1, n_sp)
    partner = me + 1 - 2 * lax.rem(me, 2)
    n_far = n_sp // CORES - 1
    has_above = me > 0
    has_below = me < n_sp - 1
    count = float(rows * n_sp * cols * group_ch)

    def peer(dist):
        return lax.rem(me + dist, n_sp)

    lat_load = pltpu.make_async_copy(lat_hbm, lat.at[:, 2 : 2 + rows], lat_sem)
    lat_load.start()

    def w_load(idx):
        src = wd_hbm if idx == 2 * w1_hbm.shape[0] else (w1_hbm, w2_hbm)[idx % 2].at[idx // 2]
        return pltpu.make_async_copy(src, raw.at[idx % 2, : 3 * kk], w_sem.at[idx % 2])

    w_load(0).start()
    w_load(1).start()

    barrier = pltpu.get_barrier_semaphore()

    @pl.loop(1, n_sp)
    def _(dist):
        pl.semaphore_signal(barrier, inc=1, device_id={axis: peer(dist)}, device_id_type=MESH_ID)

    pl.semaphore_wait(barrier, n_sp - 1)

    lat_down = pltpu.make_async_remote_copy(
        lat_hbm.at[:, rows - 2 : rows], lat.at[:, 0:2], latx_send.at[0], latx_recv.at[0], device_id={axis: below}, device_id_type=MESH_ID)
    lat_up = pltpu.make_async_remote_copy(
        lat_hbm.at[:, 0:2], lat.at[:, 2 + rows : 4 + rows], latx_send.at[1], latx_recv.at[1], device_id={axis: above}, device_id_type=MESH_ID)
    lat_down.start()
    lat_up.start()

    for col in range(N_COLS):
        bc[col] = jnp.broadcast_to(par_ref[:, col : col + 1], (chan, cols))

    lane_id_small = lax.broadcasted_iota(jnp.int32, (LATENT_PAD, cols), 1)

    def store_taps(dst, base, k, val):
        left = jnp.where(lane_id_small == 0, 0.0, pltpu.roll(val, 1, 1))
        right = jnp.where(lane_id_small == cols - 1, 0.0, pltpu.roll(val, cols - 1, 1))
        for tap, piece in enumerate((left, val, right)):
            dst[pl.ds(base + tap * LATENT_PAD, LATENT_PAD), k * cols : (k + 1) * cols] = piece.astype(BF16)

    def add_stats(acc_ref, first, k, c0, val):
        cs = pl.ds(c0, chunk)
        if first:
            acc_ref[k, cs, :] = val
            acc_ref[QUAD + k, cs, :] = val * val
        else:
            acc_ref[k, cs, :] += val
            acc_ref[QUAD + k, cs, :] += val * val

    def pack_stats(acc_ref, par, q):
        lane32 = lax.broadcasted_iota(jnp.int32, (GN_GROUPS, cols), 1)
        packed = jnp.zeros((GN_GROUPS, cols), F32)
        for idx in range(2 * QUAD):
            ref = acc_ref.at[idx]
            group = ref[pl.ds(0, GN_GROUPS, stride=group_ch), :]
            for j in range(1, group_ch):
                group = group + ref[pl.ds(j, GN_GROUPS, stride=group_ch), :]
            packed = jnp.where(lane32 == idx, jnp.sum(group, axis=1, keepdims=True), packed)
        square = jnp.concatenate([packed, jnp.zeros((cols - GN_GROUPS, cols), F32)], axis=0)
        sbuf_a[par, q] = jnp.transpose(square)[: 2 * QUAD, :]

    def pair_copy(par, q):
        return pltpu.make_async_remote_copy(
            sbuf_a.at[par, q], rbuf_a.at[par, q], sa_send.at[par, q], sa_recv.at[par, q],
            device_id={axis: partner}, device_id_type=MESH_ID)

    def add_pair(par, q):
        sbuf[par, q] = sbuf_a[par, q] + rbuf_a[par, q]

    def send_stats(par, q, first=1, last=None):
        for dist in range(first, n_far + 1 if last is None else last):
            pltpu.make_async_remote_copy(
                sbuf.at[par, q], rbuf.at[par, q, dist - 1], st_send.at[par, q], st_recv.at[par, q],
                device_id={axis: peer(CORES * dist)}, device_id_type=MESH_ID).start()

    def wait_stats(par, q):
        pair_copy(par, q).wait_send()
        whole = pltpu.make_async_remote_copy(
            rbuf.at[par, q], rbuf.at[par, q], st_send.at[par, q], st_recv.at[par, q],
            device_id={axis: below}, device_id_type=MESH_ID)
        whole.wait_send()
        whole.wait_recv()

    def make_scale(par, q, col_g, col_s, emb_idx, use_emb):
        parts = [sbuf[par, q]] + [rbuf[par, q, d] for d in range(n_far)]
        while len(parts) > 1:
            parts = [parts[i] + parts[i + 1] for i in range(0, len(parts) - 1, 2)] + ([parts[-1]] if len(parts) % 2 else [])
        total = parts[0]
        mean = total[:QUAD] / count
        var = total[QUAD:] / count - mean * mean
        inv = lax.rsqrt(var + GN_EPS)
        square = jnp.concatenate([mean, inv, jnp.zeros((cols - 2 * QUAD, cols), F32)], axis=0)
        flipped = jnp.transpose(square)[:GN_GROUPS, :]
        for k in range(QUAD):
            mean_k = jnp.broadcast_to(flipped[:, k : k + 1], (GN_GROUPS, cols))
            inv_k = jnp.broadcast_to(flipped[:, QUAD + k : QUAD + k + 1], (GN_GROUPS, cols))
            for j in range(group_ch):
                mean_b.at[k][pl.ds(j, GN_GROUPS, stride=group_ch), :] = mean_k
                inv_b.at[k][pl.ds(j, GN_GROUPS, stride=group_ch), :] = inv_k
        for k in range(QUAD):
            for c0 in range(0, chan, chunk):
                cs = pl.ds(c0, chunk)
                half_scale = inv_b[k, cs, :] * (0.5 * bc[col_g, cs, :])
                center = mean_b[k, cs, :] - jnp.where(use_emb, emb_ref[emb_idx, cs, k : k + 1], 0.0)
                scl[k, cs, :] = half_scale
                ofs[k, cs, :] = 0.5 * bc[col_s, cs, :] - center * half_scale

    def norm_row(src, q, row, dst):
        for k in range(QUAD):
            for c0 in range(0, chan, chunk):
                val = act[src, q, row, pl.ds(c0, chunk), k * cols : (k + 1) * cols].astype(F32)
                half = val * scl[k, pl.ds(c0, chunk), :] + ofs[k, pl.ds(c0, chunk), :]
                if row == 0:
                    half = jnp.where(has_above, half, 0.0)
                if row == rows + 1:
                    half = jnp.where(has_below, half, 0.0)
                store_shifts(dst, row * kk + c0, chan, k, (half + half * jnp.tanh(half)).astype(BF16))

    def halo_copies(src, q):
        down = pltpu.make_async_remote_copy(
            act.at[src, q, rows], act.at[src, q, 0], x_send.at[src, q, 0], x_recv.at[src, q, 0], device_id={axis: below}, device_id_type=MESH_ID)
        up = pltpu.make_async_remote_copy(
            act.at[src, q, 1], act.at[src, q, rows + 1], x_send.at[src, q, 1], x_recv.at[src, q, 1], device_id={axis: above}, device_id_type=MESH_ID)
        return down, up

    def send_halo(src, q):
        for copy in halo_copies(src, q):
            copy.start()

    def wait_halo(src, q):
        for copy in halo_copies(src, q):
            copy.wait()

    def out_copies(dst, q):
        return [
            pltpu.make_async_copy(act.at[0, q, 1 : 1 + rows, :, k * cols : (k + 1) * cols], dst.at[q * QUAD + k], out_sem.at[q, k])
            for k in range(QUAD)
        ]

    lat_load.wait()
    lat_down.wait()
    lat_up.wait()

    @pl.loop(0, n_quad)
    def _(q):
        @pl.when(q > 0)
        def _():
            pack_stats(stat_b, 0, q - 1)
            pair_copy(0, q - 1).start()

        for row in range(rows + 4):
            for k in range(QUAD):
                val = lat[q, row, :, k * cols : (k + 1) * cols].astype(F32)
                if row < 2:
                    val = jnp.where(has_above, val, 0.0)
                if row >= rows + 2:
                    val = jnp.where(has_below, val, 0.0)
                store_taps(xl, row * 3 * LATENT_PAD, k, val)
        for row in range(rows + 2):
            if row == 3:
                @pl.when(q > 0)
                def _():
                    pair_copy(0, q - 1).wait_recv()
                    add_pair(0, q - 1)
                    send_stats(0, q - 1)

            acc = jnp.dot(win_ref[...], xl[row * 3 * LATENT_PAD : (row + 3) * 3 * LATENT_PAD, :], preferred_element_type=F32)
            for k in range(QUAD):
                for c0 in range(0, chan, chunk):
                    val = (acc[c0 : c0 + chunk, k * cols : (k + 1) * cols] + bc[COL_BIN, c0 : c0 + chunk, :]).astype(BF16)
                    act[0, q, row, c0 : c0 + chunk, k * cols : (k + 1) * cols] = val
                    if 1 <= row <= rows:
                        add_stats(stat_b, row == 1, k, c0, val.astype(F32))
        for copy in out_copies(h0_hbm, q):
            copy.start()

    pack_stats(stat_b, 0, n_quad - 1)
    pair_copy(0, n_quad - 1).start()

    n_conv = 2 * w1_hbm.shape[0]
    n_step = n_conv * n_quad
    xbs = (xb0, xb1)
    stats = (stat_a, stat_b)
    accs = (acc_a, acc_b)
    order = (0, rows - 1) + tuple(range(1, rows - 1))

    pair_copy(0, n_quad - 1).wait_recv()
    add_pair(0, n_quad - 1)
    send_stats(0, n_quad - 1)
    wait_stats(0, 0)
    make_scale(0, 0, COL_G1, COL_S1, 0, False)
    for row in range(rows + 2):
        norm_row(0, 0, row, xb0)

    def finish(step, pos, stat):
        phase, q = step // n_quad, step % n_quad
        conv, layer = phase % 2, phase // 2
        bcol = layer + (COL_B2 - COL_B1) * conv + COL_B1
        emb = layer * n_quad + q
        row, acc = order[pos], accs[pos % 2]
        for k in range(QUAD):
            ks = slice(k * cols, (k + 1) * cols)
            for c0 in range(0, chan, chunk):
                cs = pl.ds(c0, chunk)
                val = (acc[cs, ks] + bc[bcol, cs, :]).astype(BF16).astype(F32)
                val = (jnp.where(conv == 1, act[0, q, row + 1, cs, ks].astype(F32), 0.0) + val).astype(BF16)
                act[1 - conv, q, row + 1, cs, ks] = val
                add_stats(stat, pos == 0, k, c0, val.astype(F32) + jnp.where(conv == 0, emb_ref[emb, cs, k : k + 1], 0.0))

    def start_outputs(step):
        for idx, dst in enumerate((h1_hbm, h2_hbm)):
            @pl.when(step // n_quad == 2 * idx + 1)
            def _():
                for copy in out_copies(dst, step % n_quad):
                    copy.start()

    def slot(step, side):
        phase, q = step // n_quad, step % n_quad
        conv = phase % 2
        nphase, nq = (step + 1) // n_quad, (step + 1) % n_quad
        nconv, nlayer = nphase % 2, jnp.minimum(nphase // 2, n_conv // 2 - 1)
        prev = jnp.maximum(step - 1, 0)
        pphase, pq = prev // n_quad, prev % n_quad
        ppar = (pphase + 1) % 2
        go_prev = jnp.logical_and(step > 0, pphase < n_conv - 1)
        cur, nxt = xbs[side], xbs[1 - side]
        gcol = nlayer + (COL_G2 - COL_G1) * nconv + COL_G1
        scol = nlayer + (COL_S2 - COL_S1) * nconv + COL_S1

        if side == 0:
            @pl.when(q == 0)
            def _():
                for idx in range(n_conv):
                    pl.when(phase == idx)(lambda: w_load(idx).wait())
                transpose_weight(raw.at[conv], wt)
                for idx in range(n_conv - 1):
                    pl.when(phase == idx)(lambda: w_load(idx + 2).start())

        @pl.when(conv == 1)
        def _():
            for copy in out_copies(h0_hbm, q):
                copy.wait()

        for pos, row in enumerate(order):
            if pos == 1:
                pl.when(step > 0)(lambda: start_outputs(prev))

                @pl.when(nphase < n_conv)
                def _():
                    wait_stats(nphase % 2, nq)

                @pl.when(nphase > 0)
                def _():
                    wait_halo(nconv, nq)

                make_scale(nphase % 2, nq, gcol, scol, nlayer * n_quad + nq, nconv == 1)
                pack_stats(stats[1 - side], ppar, pq)
            if pos == 2:
                @pl.when(go_prev)
                def _():
                    pair_copy(ppar, pq).start()
            if pos == 3:
                send_halo(1 - conv, q)

                @pl.when(go_prev)
                def _():
                    pair_copy(ppar, pq).wait_recv()
                    add_pair(ppar, pq)
                    send_stats(ppar, pq)
            if pos >= 2:
                half = (rows + 2) // 2
                for nrow in range(half * (pos - 2), half * (pos - 1)):
                    norm_row(nconv, nq, nrow, nxt)
            if pos == 0:
                finish(prev, rows - 1, stats[1 - side])
            else:
                finish(step, pos - 1, stats[side])
            accs[pos % 2][...] = jnp.dot(wt[:, : 3 * kk], cur[row * kk : (row + 3) * kk, :], preferred_element_type=F32)

    @pl.loop(0, n_step // 2)
    def _(pair):
        slot(2 * pair, 0)
        slot(2 * pair + 1, 1)

    finish(n_step - 1, rows - 1, stats[1])
    start_outputs(n_step - 1)

    w_load(n_conv).wait()
    transpose_weight(raw.at[n_conv % 2], wt)
    wt_out = pltpu.make_async_copy(wt, wt_hbm, wt_sem)
    wt_out.start()

    def halo_out(q):
        return pltpu.make_async_copy(act.at[0, q, 0], halo_hbm.at[q], d_sem.at[q])

    for q in range(n_quad):
        if q > 0:
            wait_halo(0, q)
        halo_out(q).start()
    for q in range(n_quad):
        halo_out(q).wait()
        for copy in out_copies(h2_hbm, q):
            copy.wait()
    wt_out.wait()


def down_kernel(
    axis, h0_hbm, h1_hbm, h2_hbm, halo_hbm, w_hbm, par_ref,
    o0_hbm, o1_hbm, o2_hbm, d_hbm,
    b0, b1, b2, halo, w, xb0, xb1, acc_a, acc_b, dbuf, bc, in_sem, halo_sem, w_sem, out_sem, d_sem,
):
    batch, rows, chan, cols = b2.shape
    n_quad = batch // QUAD
    kk = 3 * chan
    chunk = 80
    has_above = lax.axis_index(axis) > 0
    srcs, bufs, outs = (h2_hbm, h0_hbm, h1_hbm), (b2, b0, b1), (o2_hbm, o0_hbm, o1_hbm)
    xbs = (xb0, xb1)
    accs = (acc_a, acc_b)

    def load(which, q):
        part = pl.ds(q * QUAD, QUAD)
        return pltpu.make_async_copy(srcs[which].at[part], bufs[which].at[part], in_sem.at[which, q])

    def save(which, q):
        part = pl.ds(q * QUAD, QUAD)
        return pltpu.make_async_copy(bufs[which].at[part], outs[which].at[part], out_sem.at[which, q])

    def d_copy(q):
        part = pl.ds(q * QUAD, QUAD)
        return pltpu.make_async_copy(dbuf.at[part], d_hbm.at[part], d_sem.at[q])

    halo_load = pltpu.make_async_copy(halo_hbm, halo, halo_sem)
    w_load = pltpu.make_async_copy(w_hbm, w, w_sem)
    halo_load.start()
    load(0, 0).start()
    w_load.start()
    for q in range(1, n_quad):
        load(0, q).start()
    for q in range(n_quad):
        load(1, q).start()
        load(2, q).start()
    bc[...] = jnp.broadcast_to(par_ref[:, COL_BDOWN : COL_BDOWN + 1], (chan, cols))
    pick = lax.broadcasted_iota(jnp.int32, (cols // 2, cols), 1) == 2 * lax.broadcasted_iota(jnp.int32, (cols // 2, cols), 0)
    pick = pick.astype(F32).astype(BF16)

    def build(q, dst, first, last):
        for row in range(first, last):
            for k in range(QUAD):
                for c0 in range(0, chan, chunk):
                    if row == 0:
                        val = halo[q, c0 : c0 + chunk, k * cols : (k + 1) * cols]
                        val = jnp.where(has_above, val.astype(F32), 0.0).astype(BF16)
                    else:
                        val = b2[q * QUAD + k, row - 1, c0 : c0 + chunk, :]
                    store_shifts(dst, row * kk + c0, chan, k, val)

    def finish(q, row, acc):
        for k in range(QUAD):
            full = (acc[:, k * cols : (k + 1) * cols] + bc[...]).astype(BF16)
            picked = lax.dot_general(pick, full, (((1,), (1,)), ((), ())), preferred_element_type=F32)
            dbuf[q * QUAD + k, row] = picked.astype(BF16)

    def product(src, row, acc):
        acc[...] = jnp.dot(w[:, : 3 * kk], src[2 * row * kk : (2 * row + 3) * kk, :], preferred_element_type=F32)

    halo_load.wait()
    load(0, 0).wait()
    save(0, 0).start()
    build(0, xb0, 0, rows + 1)
    w_load.wait()
    half = (rows + 1) // 2

    @pl.loop(0, n_quad // 2)
    def _(pair):
        for side in range(2):
            q = 2 * pair + side
            nq = jnp.minimum(q + 1, n_quad - 1)
            pq = jnp.maximum(q - 1, 0)

            @pl.when(q + 1 < n_quad)
            def _():
                load(0, q + 1).wait()
                save(0, q + 1).start()

            for row in range(rows // 2):
                build(nq, xbs[1 - side], row * half, (row + 1) * half if row == 0 else rows + 1)
                if row == 0:
                    finish(pq, rows // 2 - 1, accs[(rows // 2 - 1) % 2])
                else:
                    finish(q, row - 1, accs[(row - 1) % 2])
                product(xbs[side], row, accs[row % 2])
                load(row + 1, q).wait()
                save(row + 1, q).start()
                if row == 0:
                    pl.when(q > 0)(lambda: d_copy(pq).start())

    finish(n_quad - 1, rows // 2 - 1, accs[(rows // 2 - 1) % 2])
    d_copy(n_quad - 1).start()

    @pl.loop(0, n_quad)
    def _(q):
        for which in range(3):
            save(which, q).wait()
        d_copy(q).wait()


def solution(mesh):
    n_sp = mesh.shape["sp"]

    def band_program(latent, time_emb, w_in, b_in, gn1_scale, gn1_shift, conv1_w, conv1_b, temb_w, temb_b, gn2_scale, gn2_shift, conv2_w, conv2_b, down_w, down_b):
        batch, rows, cols, lat_ch = latent.shape
        chan = w_in.shape[-1]
        layers = conv1_w.shape[0]
        n_quad = batch // QUAD
        lanes = QUAD * cols
        kk = 3 * chan

        lat = latent.reshape(n_quad, QUAD, rows, cols, lat_ch).transpose(0, 2, 4, 1, 3).reshape(n_quad, rows, lat_ch, lanes)
        lat = jnp.pad(lat, ((0, 0), (0, 0), (0, LATENT_PAD - lat_ch), (0, 0)))
        win = jnp.pad(w_in, ((0, 0), (0, 0), (0, LATENT_PAD - lat_ch), (0, 0))).reshape(9 * LATENT_PAD, chan).T
        w1, w2, wd = conv1_w.reshape(layers, 9 * chan, chan), conv2_w.reshape(layers, 9 * chan, chan), down_w.reshape(9 * chan, chan)
        padded = 128 * pl.cdiv(9 * chan, 128)
        par = jnp.concatenate([b_in[None], gn1_scale, gn1_shift, conv1_b, gn2_scale, gn2_shift, conv2_b, down_b[None]], axis=0).astype(F32).T
        emb_act = jax.nn.silu(time_emb.astype(F32)).astype(BF16)
        emb = jnp.einsum("bt,ltc->lbc", emb_act, temb_w, preferred_element_type=F32) + temb_b.astype(F32)[:, None, :]
        emb = emb.reshape(layers * n_quad, QUAD, chan).transpose(0, 2, 1)
        band = jax.ShapeDtypeStruct((batch, rows, chan, cols), BF16)
        hbm = pl.BlockSpec(memory_space=pl.ANY)
        vmem = pl.BlockSpec(memory_space=pltpu.VMEM)
        dma = pltpu.SemaphoreType.DMA
        h0, h1, h2, halo, wt = pl.pallas_call(
            functools.partial(band_kernel, n_sp, "sp"),
            out_shape=(band, band, band, jax.ShapeDtypeStruct((n_quad, chan, lanes), BF16), jax.ShapeDtypeStruct((chan, padded), BF16)),
            in_specs=[hbm, vmem, hbm, hbm, hbm, vmem, vmem],
            out_specs=(hbm,) * 5,
            scratch_shapes=[
                pltpu.VMEM((n_quad, rows + 4, LATENT_PAD, lanes), BF16),
                pltpu.VMEM(((rows + 4) * 3 * LATENT_PAD, lanes), BF16),
                pltpu.VMEM((2, n_quad, rows + 2, chan, lanes), BF16),
                pltpu.VMEM(((rows + 2) * kk, lanes), BF16),
                pltpu.VMEM(((rows + 2) * kk, lanes), BF16),
                pltpu.VMEM((2, padded, chan), BF16),
                pltpu.VMEM((chan, padded), BF16),
                pltpu.VMEM((chan, lanes), F32),
                pltpu.VMEM((chan, lanes), F32),
                pltpu.VMEM((N_COLS, chan, cols), F32),
                pltpu.VMEM((2 * QUAD, chan, cols), F32),
                pltpu.VMEM((2 * QUAD, chan, cols), F32),
                pltpu.VMEM((QUAD, chan, cols), F32),
                pltpu.VMEM((QUAD, chan, cols), F32),
                pltpu.VMEM((QUAD, chan, cols), F32),
                pltpu.VMEM((QUAD, chan, cols), F32),
                pltpu.VMEM((2, n_quad, 2 * QUAD, cols), F32),
                pltpu.VMEM((2, n_quad, 2 * QUAD, cols), F32),
                pltpu.VMEM((2, n_quad, 2 * QUAD, cols), F32),
                pltpu.VMEM((2, n_quad, n_sp // CORES - 1, 2 * QUAD, cols), F32),
                dma, dma((2,)), dma, dma((n_quad, QUAD)), dma((n_quad,)),
                dma((2,)), dma((2,)), dma((2, n_quad)), dma((2, n_quad)), dma((2, n_quad)), dma((2, n_quad)),
                dma((2, n_quad, 2)), dma((2, n_quad, 2)),
            ],
            compiler_params=pltpu.CompilerParams(collective_id=0, has_side_effects=True, vmem_limit_bytes=60 * 1024 * 1024),
            name="band",
        )(lat, win, w1, w2, wd, par, emb)
        h0, h1, h2, d = pl.pallas_call(
            functools.partial(down_kernel, "sp"),
            out_shape=(band, band, band, jax.ShapeDtypeStruct((batch, rows // 2, cols // 2, chan), BF16)),
            in_specs=[hbm] * 5 + [vmem],
            out_specs=(hbm,) * 4,
            scratch_shapes=[
                pltpu.VMEM(band.shape, BF16), pltpu.VMEM(band.shape, BF16), pltpu.VMEM(band.shape, BF16),
                pltpu.VMEM((n_quad, chan, lanes), BF16),
                pltpu.VMEM((chan, padded), BF16),
                pltpu.VMEM(((rows + 1) * kk, lanes), BF16),
                pltpu.VMEM(((rows + 1) * kk, lanes), BF16),
                pltpu.VMEM((chan, lanes), F32),
                pltpu.VMEM((chan, lanes), F32),
                pltpu.VMEM((batch, rows // 2, cols // 2, chan), BF16),
                pltpu.VMEM((chan, cols), F32),
                dma((3, n_quad)), dma, dma, dma((3, n_quad)), dma((n_quad,)),
            ],
            compiler_params=pltpu.CompilerParams(vmem_limit_bytes=60 * 1024 * 1024),
            name="down",
        )(h0, h1, h2, halo, wt, par)
        return tuple(h.transpose(0, 1, 3, 2) for h in (h0, h1, h2)) + (d,)

    band_spec = P("dp", "sp", None, None)
    return jax.shard_map(band_program, mesh=mesh, in_specs=(band_spec, P("dp", None)) + (P(),) * 14, out_specs=(band_spec,) * 4, check_vma=False)
```

```python
import functools

import jax
import jax.numpy as jnp
from jax import lax
from jax.experimental import pallas as pl
from jax.experimental.pallas import tpu as pltpu
from jax.sharding import PartitionSpec as P

GN_GROUPS = 32
GN_EPS = 1e-5
QUAD = 4
LATENT_PAD = 16
CORES = 2
MESH_ID = pl.DeviceIdType.MESH
F32 = jnp.float32
BF16 = jnp.bfloat16

COL_BIN = 0
COL_G1, COL_S1, COL_B1, COL_G2, COL_S2, COL_B2 = 1, 3, 5, 7, 9, 11
COL_BDOWN = 13
N_COLS = 13


def store_shifts(dst, base, stride, k, val):
    size, cols = val.shape
    lane = lax.broadcasted_iota(jnp.int32, val.shape, 1)
    zero = jnp.zeros_like(val)
    left = jnp.where(lane == 0, zero, pltpu.roll(val, 1, 1))
    right = jnp.where(lane == cols - 1, zero, pltpu.roll(val, cols - 1, 1))
    for tap, piece in enumerate((left, val, right)):
        dst[base + tap * stride : base + tap * stride + size, k * cols : (k + 1) * cols] = piece


def transpose_weight(raw, out):
    for start in range(0, out.shape[1], 128):
        out[:, start : start + 128] = jnp.transpose(raw[start : start + 128, :])


def band_kernel(
    n_sp, axis,
    lat_hbm, win_ref, w1_hbm, w2_hbm, wd_hbm, par_ref, emb_in,
    h0_hbm, h1_hbm, h2_hbm, halo_hbm, wt_hbm,
    lat, xl, act, xb0, xb1, raw, wt, acc_a, acc_b, emb_ref, bc, stat_a, stat_b, scl, ofs, inv_b, mean_b, sbuf_a, rbuf_a, sbuf, rbuf,
    lat_sem, w_sem, wt_sem, out_sem, d_sem, latx_send, latx_recv, sa_send, sa_recv, st_send, st_recv, x_send, x_recv,
):
    _, n_quad, _, chan, lanes = act.shape
    cols = lanes // QUAD
    group_ch = chan // GN_GROUPS
    kk = 3 * chan
    rows = h0_hbm.shape[1]
    chunk = 80
    me = lax.axis_index(axis)
    above = lax.rem(me + n_sp - 1, n_sp)
    below = lax.rem(me + 1, n_sp)
    partner = me + 1 - 2 * lax.rem(me, 2)
    n_far = n_sp // CORES - 1
    has_above = me > 0
    has_below = me < n_sp - 1
    count = float(rows * n_sp * cols * group_ch)

    def peer(dist):
        return lax.rem(me + dist, n_sp)

    lat_load = pltpu.make_async_copy(lat_hbm, lat.at[:, 2 : 2 + rows], lat_sem)
    lat_load.start()

    def w_load(idx):
        src = wd_hbm if idx == 2 * w1_hbm.shape[0] else (w1_hbm, w2_hbm)[idx % 2].at[idx // 2]
        return pltpu.make_async_copy(src, raw.at[idx % 2, : 3 * kk], w_sem.at[idx % 2])

    w_load(0).start()
    w_load(1).start()

    barrier = pltpu.get_barrier_semaphore()

    @pl.loop(1, n_sp)
    def _(dist):
        pl.semaphore_signal(barrier, inc=1, device_id={axis: peer(dist)}, device_id_type=MESH_ID)

    pl.semaphore_wait(barrier, n_sp - 1)

    lat_down = pltpu.make_async_remote_copy(
        lat_hbm.at[:, rows - 2 : rows], lat.at[:, 0:2], latx_send.at[0], latx_recv.at[0], device_id={axis: below}, device_id_type=MESH_ID)
    lat_up = pltpu.make_async_remote_copy(
        lat_hbm.at[:, 0:2], lat.at[:, 2 + rows : 4 + rows], latx_send.at[1], latx_recv.at[1], device_id={axis: above}, device_id_type=MESH_ID)
    lat_down.start()
    lat_up.start()

    for col in range(N_COLS):
        bc[col] = jnp.broadcast_to(par_ref[:, col : col + 1], (chan, cols))
    for lay in range(emb_in.shape[0]):
        for quad in range(n_quad):
            emb_ref[lay * n_quad + quad] = emb_in[lay, :, quad * QUAD : (quad + 1) * QUAD]

    lane_id_small = lax.broadcasted_iota(jnp.int32, (LATENT_PAD, cols), 1)

    def store_taps(dst, base, k, val):
        left = jnp.where(lane_id_small == 0, 0.0, pltpu.roll(val, 1, 1))
        right = jnp.where(lane_id_small == cols - 1, 0.0, pltpu.roll(val, cols - 1, 1))
        for tap, piece in enumerate((left, val, right)):
            dst[pl.ds(base + tap * LATENT_PAD, LATENT_PAD), k * cols : (k + 1) * cols] = piece.astype(BF16)

    def add_stats(acc_ref, first, k, c0, val):
        cs = pl.ds(c0, chunk)
        if first:
            acc_ref[k, cs, :] = val
            acc_ref[QUAD + k, cs, :] = val * val
        else:
            acc_ref[k, cs, :] += val
            acc_ref[QUAD + k, cs, :] += val * val

    def pack_stats(acc_ref, par, q):
        lane32 = lax.broadcasted_iota(jnp.int32, (GN_GROUPS, cols), 1)
        packed = jnp.zeros((GN_GROUPS, cols), F32)
        for idx in range(2 * QUAD):
            ref = acc_ref.at[idx]
            group = ref[pl.ds(0, GN_GROUPS, stride=group_ch), :]
            for j in range(1, group_ch):
                group = group + ref[pl.ds(j, GN_GROUPS, stride=group_ch), :]
            packed = jnp.where(lane32 == idx, jnp.sum(group, axis=1, keepdims=True), packed)
        square = jnp.concatenate([packed, jnp.zeros((cols - GN_GROUPS, cols), F32)], axis=0)
        sbuf_a[par, q] = jnp.transpose(square)[: 2 * QUAD, :]

    def pair_copy(par, q):
        return pltpu.make_async_remote_copy(
            sbuf_a.at[par, q], rbuf_a.at[par, q], sa_send.at[par, q], sa_recv.at[par, q],
            device_id={axis: partner}, device_id_type=MESH_ID)

    def add_pair(par, q):
        sbuf[par, q] = sbuf_a[par, q] + rbuf_a[par, q]

    def send_stats(par, q, first=1, last=None):
        for dist in range(first, n_far + 1 if last is None else last):
            pltpu.make_async_remote_copy(
                sbuf.at[par, q], rbuf.at[par, q, dist - 1], st_send.at[par, q], st_recv.at[par, q],
                device_id={axis: peer(CORES * dist)}, device_id_type=MESH_ID).start()

    def wait_stats(par, q):
        pair_copy(par, q).wait_send()
        whole = pltpu.make_async_remote_copy(
            rbuf.at[par, q], rbuf.at[par, q], st_send.at[par, q], st_recv.at[par, q],
            device_id={axis: below}, device_id_type=MESH_ID)
        whole.wait_send()
        whole.wait_recv()

    def make_scale(par, q, col_g, col_s, emb_idx, use_emb):
        parts = [sbuf[par, q]] + [rbuf[par, q, d] for d in range(n_far)]
        while len(parts) > 1:
            parts = [parts[i] + parts[i + 1] for i in range(0, len(parts) - 1, 2)] + ([parts[-1]] if len(parts) % 2 else [])
        total = parts[0]
        mean = total[:QUAD] / count
        var = total[QUAD:] / count - mean * mean
        inv = lax.rsqrt(var + GN_EPS)
        square = jnp.concatenate([mean, inv, jnp.zeros((cols - 2 * QUAD, cols), F32)], axis=0)
        flipped = jnp.transpose(square)[:GN_GROUPS, :]
        for k in range(QUAD):
            mean_k = jnp.broadcast_to(flipped[:, k : k + 1], (GN_GROUPS, cols))
            inv_k = jnp.broadcast_to(flipped[:, QUAD + k : QUAD + k + 1], (GN_GROUPS, cols))
            for j in range(group_ch):
                mean_b.at[k][pl.ds(j, GN_GROUPS, stride=group_ch), :] = mean_k
                inv_b.at[k][pl.ds(j, GN_GROUPS, stride=group_ch), :] = inv_k
        for k in range(QUAD):
            for c0 in range(0, chan, chunk):
                cs = pl.ds(c0, chunk)
                half_scale = inv_b[k, cs, :] * (0.5 * bc[col_g, cs, :])
                center = mean_b[k, cs, :] - jnp.where(use_emb, emb_ref[emb_idx, cs, k : k + 1], 0.0)
                scl[k, cs, :] = half_scale
                ofs[k, cs, :] = 0.5 * bc[col_s, cs, :] - center * half_scale

    def norm_row(src, q, row, dst):
        for k in range(QUAD):
            for c0 in range(0, chan, chunk):
                val = act[src, q, row, pl.ds(c0, chunk), k * cols : (k + 1) * cols].astype(F32)
                half = val * scl[k, pl.ds(c0, chunk), :] + ofs[k, pl.ds(c0, chunk), :]
                if row == 0:
                    half = jnp.where(has_above, half, 0.0)
                if row == rows + 1:
                    half = jnp.where(has_below, half, 0.0)
                store_shifts(dst, row * kk + c0, chan, k, (half + half * jnp.tanh(half)).astype(BF16))

    def halo_copies(src, q):
        down = pltpu.make_async_remote_copy(
            act.at[src, q, rows], act.at[src, q, 0], x_send.at[src, q, 0], x_recv.at[src, q, 0], device_id={axis: below}, device_id_type=MESH_ID)
        up = pltpu.make_async_remote_copy(
            act.at[src, q, 1], act.at[src, q, rows + 1], x_send.at[src, q, 1], x_recv.at[src, q, 1], device_id={axis: above}, device_id_type=MESH_ID)
        return down, up

    def send_halo(src, q):
        for copy in halo_copies(src, q):
            copy.start()

    def wait_halo(src, q):
        for copy in halo_copies(src, q):
            copy.wait()

    def out_copies(dst, q):
        return [
            pltpu.make_async_copy(act.at[0, q, 1 : 1 + rows, :, k * cols : (k + 1) * cols], dst.at[q * QUAD + k], out_sem.at[q, k])
            for k in range(QUAD)
        ]

    lat_load.wait()
    lat_down.wait()
    lat_up.wait()

    @pl.loop(0, n_quad)
    def _(q):
        @pl.when(q > 0)
        def _():
            pack_stats(stat_b, 0, q - 1)
            pair_copy(0, q - 1).start()

        for row in range(rows + 4):
            for k in range(QUAD):
                val = lat[q, row, :, k * cols : (k + 1) * cols].astype(F32)
                if row < 2:
                    val = jnp.where(has_above, val, 0.0)
                if row >= rows + 2:
                    val = jnp.where(has_below, val, 0.0)
                store_taps(xl, row * 3 * LATENT_PAD, k, val)
        for row in range(rows + 2):
            if row == 3:
                @pl.when(q > 0)
                def _():
                    pair_copy(0, q - 1).wait_recv()
                    add_pair(0, q - 1)
                    send_stats(0, q - 1)

            acc = jnp.dot(win_ref[...], xl[row * 3 * LATENT_PAD : (row + 3) * 3 * LATENT_PAD, :], preferred_element_type=F32)
            for k in range(QUAD):
                for c0 in range(0, chan, chunk):
                    val = (acc[c0 : c0 + chunk, k * cols : (k + 1) * cols] + bc[COL_BIN, c0 : c0 + chunk, :]).astype(BF16)
                    act[0, q, row, c0 : c0 + chunk, k * cols : (k + 1) * cols] = val
                    if 1 <= row <= rows:
                        add_stats(stat_b, row == 1, k, c0, val.astype(F32))
        for copy in out_copies(h0_hbm, q):
            copy.start()

    pack_stats(stat_b, 0, n_quad - 1)
    pair_copy(0, n_quad - 1).start()

    n_conv = 2 * w1_hbm.shape[0]
    n_step = n_conv * n_quad
    xbs = (xb0, xb1)
    stats = (stat_a, stat_b)
    accs = (acc_a, acc_b)
    order = (0, rows - 1) + tuple(range(1, rows - 1))

    pair_copy(0, n_quad - 1).wait_recv()
    add_pair(0, n_quad - 1)
    send_stats(0, n_quad - 1)
    wait_stats(0, 0)
    make_scale(0, 0, COL_G1, COL_S1, 0, False)
    for row in range(rows + 2):
        norm_row(0, 0, row, xb0)

    def finish(step, pos, stat):
        phase, q = step // n_quad, step % n_quad
        conv, layer = phase % 2, phase // 2
        bcol = layer + (COL_B2 - COL_B1) * conv + COL_B1
        emb = layer * n_quad + q
        row, acc = order[pos], accs[pos % 2]
        for k in range(QUAD):
            ks = slice(k * cols, (k + 1) * cols)
            for c0 in range(0, chan, chunk):
                cs = pl.ds(c0, chunk)
                val = (acc[cs, ks] + bc[bcol, cs, :]).astype(BF16).astype(F32)
                val = (jnp.where(conv == 1, act[0, q, row + 1, cs, ks].astype(F32), 0.0) + val).astype(BF16)
                act[1 - conv, q, row + 1, cs, ks] = val
                add_stats(stat, pos == 0, k, c0, val.astype(F32) + jnp.where(conv == 0, emb_ref[emb, cs, k : k + 1], 0.0))

    def start_outputs(step):
        for idx, dst in enumerate((h1_hbm, h2_hbm)):
            @pl.when(step // n_quad == 2 * idx + 1)
            def _():
                for copy in out_copies(dst, step % n_quad):
                    copy.start()

    def slot(step, side):
        phase, q = step // n_quad, step % n_quad
        conv = phase % 2
        nphase, nq = (step + 1) // n_quad, (step + 1) % n_quad
        nconv, nlayer = nphase % 2, jnp.minimum(nphase // 2, n_conv // 2 - 1)
        prev = jnp.maximum(step - 1, 0)
        pphase, pq = prev // n_quad, prev % n_quad
        ppar = (pphase + 1) % 2
        go_prev = jnp.logical_and(step > 0, pphase < n_conv - 1)
        cur, nxt = xbs[side], xbs[1 - side]
        gcol = nlayer + (COL_G2 - COL_G1) * nconv + COL_G1
        scol = nlayer + (COL_S2 - COL_S1) * nconv + COL_S1

        if side == 0:
            @pl.when(q == 0)
            def _():
                for idx in range(n_conv):
                    pl.when(phase == idx)(lambda: w_load(idx).wait())
                transpose_weight(raw.at[conv], wt)
                for idx in range(n_conv - 1):
                    pl.when(phase == idx)(lambda: w_load(idx + 2).start())

        @pl.when(conv == 1)
        def _():
            for copy in out_copies(h0_hbm, q):
                copy.wait()

        @pl.when(nphase < n_conv)
        def _():
            wait_stats(nphase % 2, nq)

        @pl.when(nphase > 0)
        def _():
            wait_halo(nconv, nq)

        share = (rows + 2) // (rows - 1)
        for pos, row in enumerate(order):
            if pos == 1:
                pl.when(step > 0)(lambda: start_outputs(prev))
                pl.when(go_prev)(lambda: pair_copy(ppar, pq).start())
            if pos == 2:
                @pl.when(go_prev)
                def _():
                    pair_copy(ppar, pq).wait_recv()
                    add_pair(ppar, pq)
                    send_stats(ppar, pq)
            if pos == 3:
                send_halo(1 - conv, q)
            if pos == 0:
                finish(prev, rows - 1, stats[1 - side])
                pack_stats(stats[1 - side], ppar, pq)
                make_scale(nphase % 2, nq, gcol, scol, nlayer * n_quad + nq, nconv == 1)
            else:
                finish(step, pos - 1, stats[side])
                for nrow in range(share * (pos - 1), share * pos):
                    norm_row(nconv, nq, nrow, nxt)
            accs[pos % 2][...] = jnp.dot(wt[:, : 3 * kk], cur[row * kk : (row + 3) * kk, :], preferred_element_type=F32)

    @pl.loop(0, n_step // 2)
    def _(pair):
        slot(2 * pair, 0)
        slot(2 * pair + 1, 1)

    finish(n_step - 1, rows - 1, stats[1])
    start_outputs(n_step - 1)

    w_load(n_conv).wait()
    transpose_weight(raw.at[n_conv % 2], wt)
    wt_out = pltpu.make_async_copy(wt, wt_hbm, wt_sem)
    wt_out.start()

    def halo_out(q):
        return pltpu.make_async_copy(act.at[0, q, 0], halo_hbm.at[q], d_sem.at[q])

    for q in range(n_quad):
        if q > 0:
            wait_halo(0, q)
        halo_out(q).start()
    for q in range(n_quad):
        halo_out(q).wait()
        for copy in out_copies(h2_hbm, q):
            copy.wait()
    wt_out.wait()


def down_kernel(
    axis, h0_hbm, h1_hbm, h2_hbm, halo_hbm, w_hbm, par_ref,
    o0_hbm, o1_hbm, o2_hbm, d_hbm,
    b0, b1, b2, halo, w, xb0, xb1, acc_a, acc_b, dbuf, bc, in_sem, halo_sem, w_sem, out_sem, d_sem,
):
    batch, rows, chan, cols = b2.shape
    n_quad = batch // QUAD
    kk = 3 * chan
    chunk = 80
    has_above = lax.axis_index(axis) > 0
    srcs, bufs, outs = (h2_hbm, h0_hbm, h1_hbm), (b2, b0, b1), (o2_hbm, o0_hbm, o1_hbm)
    xbs = (xb0, xb1)
    accs = (acc_a, acc_b)

    def load(which, q):
        part = pl.ds(q * QUAD, QUAD)
        return pltpu.make_async_copy(srcs[which].at[part], bufs[which].at[part], in_sem.at[which, q])

    def save(which, q):
        part = pl.ds(q * QUAD, QUAD)
        return pltpu.make_async_copy(bufs[which].at[part], outs[which].at[part], out_sem.at[which, q])

    def d_copy(q):
        part = pl.ds(q * QUAD, QUAD)
        return pltpu.make_async_copy(dbuf.at[part], d_hbm.at[part], d_sem.at[q])

    halo_load = pltpu.make_async_copy(halo_hbm, halo, halo_sem)
    w_load = pltpu.make_async_copy(w_hbm, w, w_sem)
    halo_load.start()
    load(0, 0).start()
    w_load.start()
    for q in range(1, n_quad):
        load(0, q).start()
    for q in range(n_quad):
        load(1, q).start()
        load(2, q).start()
    bc[...] = jnp.broadcast_to(par_ref[:, COL_BDOWN : COL_BDOWN + 1], (chan, cols))
    pick = lax.broadcasted_iota(jnp.int32, (cols // 2, cols), 1) == 2 * lax.broadcasted_iota(jnp.int32, (cols // 2, cols), 0)
    pick = pick.astype(F32).astype(BF16)

    def build(q, dst, first, last):
        for row in range(first, last):
            for k in range(QUAD):
                for c0 in range(0, chan, chunk):
                    if row == 0:
                        val = halo[q, c0 : c0 + chunk, k * cols : (k + 1) * cols]
                        val = jnp.where(has_above, val.astype(F32), 0.0).astype(BF16)
                    else:
                        val = b2[q * QUAD + k, row - 1, c0 : c0 + chunk, :]
                    store_shifts(dst, row * kk + c0, chan, k, val)

    def finish(q, row, acc):
        for k in range(QUAD):
            full = (acc[:, k * cols : (k + 1) * cols] + bc[...]).astype(BF16)
            picked = lax.dot_general(pick, full, (((1,), (1,)), ((), ())), preferred_element_type=F32)
            dbuf[q * QUAD + k, row] = picked.astype(BF16)

    def product(src, row, acc):
        acc[...] = jnp.dot(w[:, : 3 * kk], src[2 * row * kk : (2 * row + 3) * kk, :], preferred_element_type=F32)

    halo_load.wait()
    load(0, 0).wait()
    save(0, 0).start()
    build(0, xb0, 0, rows + 1)
    w_load.wait()
    half = (rows + 1) // 2

    @pl.loop(0, n_quad // 2)
    def _(pair):
        for side in range(2):
            q = 2 * pair + side
            nq = jnp.minimum(q + 1, n_quad - 1)
            pq = jnp.maximum(q - 1, 0)

            @pl.when(q + 1 < n_quad)
            def _():
                load(0, q + 1).wait()
                save(0, q + 1).start()

            for row in range(rows // 2):
                build(nq, xbs[1 - side], row * half, (row + 1) * half if row == 0 else rows + 1)
                if row == 0:
                    finish(pq, rows // 2 - 1, accs[(rows // 2 - 1) % 2])
                else:
                    finish(q, row - 1, accs[(row - 1) % 2])
                product(xbs[side], row, accs[row % 2])
                load(row + 1, q).wait()
                save(row + 1, q).start()
                if row == 0:
                    pl.when(q > 0)(lambda: d_copy(pq).start())

    finish(n_quad - 1, rows // 2 - 1, accs[(rows // 2 - 1) % 2])
    d_copy(n_quad - 1).start()

    @pl.loop(0, n_quad)
    def _(q):
        for which in range(3):
            save(which, q).wait()
        d_copy(q).wait()


def solution(mesh):
    n_sp = mesh.shape["sp"]

    def band_program(latent, time_emb, w_in, b_in, gn1_scale, gn1_shift, conv1_w, conv1_b, temb_w, temb_b, gn2_scale, gn2_shift, conv2_w, conv2_b, down_w, down_b):
        batch, rows, cols, lat_ch = latent.shape
        chan = w_in.shape[-1]
        layers = conv1_w.shape[0]
        n_quad = batch // QUAD
        lanes = QUAD * cols
        kk = 3 * chan

        lat = latent.reshape(n_quad, QUAD, rows, cols, lat_ch).transpose(0, 2, 4, 1, 3).reshape(n_quad, rows, lat_ch, lanes)
        lat = jnp.pad(lat, ((0, 0), (0, 0), (0, LATENT_PAD - lat_ch), (0, 0)))
        win = jnp.pad(w_in, ((0, 0), (0, 0), (0, LATENT_PAD - lat_ch), (0, 0))).reshape(9 * LATENT_PAD, chan).T
        w1, w2, wd = conv1_w.reshape(layers, 9 * chan, chan), conv2_w.reshape(layers, 9 * chan, chan), down_w.reshape(9 * chan, chan)
        padded = 128 * pl.cdiv(9 * chan, 128)
        par = jnp.concatenate([b_in[None], gn1_scale, gn1_shift, conv1_b, gn2_scale, gn2_shift, conv2_b, down_b[None]], axis=0).astype(F32).T
        emb_act = jax.nn.silu(time_emb.astype(F32)).astype(BF16)
        emb = jnp.einsum("ltc,bt->lcb", temb_w, emb_act, preferred_element_type=F32) + temb_b.astype(F32)[:, :, None]
        band = jax.ShapeDtypeStruct((batch, rows, chan, cols), BF16)
        hbm = pl.BlockSpec(memory_space=pl.ANY)
        vmem = pl.BlockSpec(memory_space=pltpu.VMEM)
        dma = pltpu.SemaphoreType.DMA
        h0, h1, h2, halo, wt = pl.pallas_call(
            functools.partial(band_kernel, n_sp, "sp"),
            out_shape=(band, band, band, jax.ShapeDtypeStruct((n_quad, chan, lanes), BF16), jax.ShapeDtypeStruct((chan, padded), BF16)),
            in_specs=[hbm, vmem, hbm, hbm, hbm, vmem, vmem],
            out_specs=(hbm,) * 5,
            scratch_shapes=[
                pltpu.VMEM((n_quad, rows + 4, LATENT_PAD, lanes), BF16),
                pltpu.VMEM(((rows + 4) * 3 * LATENT_PAD, lanes), BF16),
                pltpu.VMEM((2, n_quad, rows + 2, chan, lanes), BF16),
                pltpu.VMEM(((rows + 2) * kk, lanes), BF16),
                pltpu.VMEM(((rows + 2) * kk, lanes), BF16),
                pltpu.VMEM((2, padded, chan), BF16),
                pltpu.VMEM((chan, padded), BF16),
                pltpu.VMEM((chan, lanes), F32),
                pltpu.VMEM((chan, lanes), F32),
                pltpu.VMEM((layers * n_quad, chan, QUAD), F32),
                pltpu.VMEM((N_COLS, chan, cols), F32),
                pltpu.VMEM((2 * QUAD, chan, cols), F32),
                pltpu.VMEM((2 * QUAD, chan, cols), F32),
                pltpu.VMEM((QUAD, chan, cols), F32),
                pltpu.VMEM((QUAD, chan, cols), F32),
                pltpu.VMEM((QUAD, chan, cols), F32),
                pltpu.VMEM((QUAD, chan, cols), F32),
                pltpu.VMEM((2, n_quad, 2 * QUAD, cols), F32),
                pltpu.VMEM((2, n_quad, 2 * QUAD, cols), F32),
                pltpu.VMEM((2, n_quad, 2 * QUAD, cols), F32),
                pltpu.VMEM((2, n_quad, n_sp // CORES - 1, 2 * QUAD, cols), F32),
                dma, dma((2,)), dma, dma((n_quad, QUAD)), dma((n_quad,)),
                dma((2,)), dma((2,)), dma((2, n_quad)), dma((2, n_quad)), dma((2, n_quad)), dma((2, n_quad)),
                dma((2, n_quad, 2)), dma((2, n_quad, 2)),
            ],
            compiler_params=pltpu.CompilerParams(collective_id=0, has_side_effects=True, vmem_limit_bytes=60 * 1024 * 1024),
            name="band",
        )(lat, win, w1, w2, wd, par, emb)
        h0, h1, h2, d = pl.pallas_call(
            functools.partial(down_kernel, "sp"),
            out_shape=(band, band, band, jax.ShapeDtypeStruct((batch, rows // 2, cols // 2, chan), BF16)),
            in_specs=[hbm] * 5 + [vmem],
            out_specs=(hbm,) * 4,
            scratch_shapes=[
                pltpu.VMEM(band.shape, BF16), pltpu.VMEM(band.shape, BF16), pltpu.VMEM(band.shape, BF16),
                pltpu.VMEM((n_quad, chan, lanes), BF16),
                pltpu.VMEM((chan, padded), BF16),
                pltpu.VMEM(((rows + 1) * kk, lanes), BF16),
                pltpu.VMEM(((rows + 1) * kk, lanes), BF16),
                pltpu.VMEM((chan, lanes), F32),
                pltpu.VMEM((chan, lanes), F32),
                pltpu.VMEM((batch, rows // 2, cols // 2, chan), BF16),
                pltpu.VMEM((chan, cols), F32),
                dma((3, n_quad)), dma, dma, dma((3, n_quad)), dma((n_quad,)),
            ],
            compiler_params=pltpu.CompilerParams(vmem_limit_bytes=60 * 1024 * 1024),
            name="down",
        )(h0, h1, h2, halo, wt, par)
        return tuple(h.transpose(0, 1, 3, 2) for h in (h0, h1, h2)) + (d,)

    band_spec = P("dp", "sp", None, None)
    return jax.shard_map(band_program, mesh=mesh, in_specs=(band_spec, P("dp", None)) + (P(),) * 14, out_specs=(band_spec,) * 4, check_vma=False)
```
